32 devices in a mesh: batch: 8 (over z, y), space: 4 (over x, core).
Axes of the slice: x: 2, y: 2, z: 4, core: 2. Of those that a mesh axis runs over, the one named last changes fastest.
Arguments:
- features: bfloat16 [8, 48, 72, 1024], P('batch', 'space'), may hold values from -600 to 600
- depth_one: bfloat16 [3, 3, 1024], replicated, may hold values from -2 to 2
- gain_one: float32 [1024], replicated, may hold values from 0.25 to 1.75
- shift_one: float32 [1024], replicated, may hold values from -3 to 3
- point_one: bfloat16 [1024, 1536], replicated, may hold values from -0.1875 to 0.1875
- gain_two: float32 [1536], replicated, may hold values from 0.25 to 1.75
- shift_two: float32 [1536], replicated, may hold values from -3 to 3
- depth_two: bfloat16 [3, 3, 1536], replicated, may hold values from -2 to 2
- gain_three: float32 [1536], replicated, may hold values from 0.25 to 1.75
- shift_three: float32 [1536], replicated, may hold values from -3 to 3
- point_two: bfloat16 [1536, 2048], replicated, may hold values from -0.15625 to 0.15625
- gain_four: float32 [2048], replicated, may hold values from 0.25 to 1.75
- shift_four: float32 [2048], replicated, may hold values from -3 to 3
Outputs:
- exit_map: bfloat16 [8, 48, 72, 2048], P('batch', 'space')
The draws below stay inside these ranges and needn't reach their ends.
All inputs are finite; a program needn't handle non-finite values.
Results may differ from the reference program's by a relative error of at most 0.0079.
Values may be sent and summed in bfloat16 or wider, within the bound.
A program may use at most 64 MiB of HBM per device.

```python
import jax
import jax.numpy as jnp
from jax import lax

CH_IN = 1024
CH_MID = 1536
CH_OUT = 2048
COLS = 72
RATE = 2
LATS = 48
SAMPLES = 8


def draw_features(key, part):
    key_base, key_chan = jax.random.split(key, 2)
    sample_ramp = 3.0 ** (jnp.arange(SAMPLES, dtype=jnp.float32) / max(SAMPLES - 1, 1))
    row_ramp = 3.0 ** (jnp.arange(LATS, dtype=jnp.float32) / max(LATS - 1, 1))
    base = jnp.clip(jax.random.normal(key_base, (SAMPLES, LATS, COLS, CH_IN), jnp.float32), -6.0, 6.0)
    channel_scale = jax.random.uniform(key_chan, (CH_IN,), jnp.float32, 0.5, 2.0)
    values = base * sample_ramp[:, None, None, None] * row_ramp[None, :, None, None] * channel_scale
    return values.astype(jnp.bfloat16)


def bell_draw(stream_key, shape, deviation, limit, kind=jnp.bfloat16):
    entries = jax.random.normal(stream_key, shape, jnp.float32) * deviation
    return jnp.minimum(jnp.maximum(entries, -limit), limit).astype(kind)


def setup_inputs(seed: int = 0) -> dict:
    seeds = jax.random.split(jax.random.key(seed), 14)
    features = draw_features(jax.random.fold_in(seeds[13], 71), 0)
    depth_one = bell_draw(seeds[1], (3, 3, CH_IN), 9 ** -0.5, 2.0)
    gain_one = jnp.clip(1.0 + 0.15 * jax.random.normal(seeds[2], (CH_IN,), jnp.float32), 0.25, 1.75)
    shift_one = bell_draw(seeds[3], (CH_IN,), 0.5, 3.0, jnp.float32)
    point_one = bell_draw(seeds[4], (CH_IN, CH_MID), CH_IN ** -0.5, 0.1875)
    gain_two = jnp.clip(1.0 + 0.15 * jax.random.normal(seeds[5], (CH_MID,), jnp.float32), 0.25, 1.75)
    shift_two = bell_draw(seeds[6], (CH_MID,), 0.5, 3.0, jnp.float32)
    depth_two = bell_draw(seeds[7], (3, 3, CH_MID), 9 ** -0.5, 2.0)
    gain_three = jnp.clip(1.0 + 0.15 * jax.random.normal(seeds[8], (CH_MID,), jnp.float32), 0.25, 1.75)
    shift_three = bell_draw(seeds[9], (CH_MID,), 0.5, 3.0, jnp.float32)
    point_two = bell_draw(seeds[10], (CH_MID, CH_OUT), CH_MID ** -0.5, 0.15625)
    gain_four = jnp.clip(1.0 + 0.15 * jax.random.normal(seeds[11], (CH_OUT,), jnp.float32), 0.25, 1.75)
    shift_four = bell_draw(seeds[12], (CH_OUT,), 0.5, 3.0, jnp.float32)
    return {"features": features, "depth_one": depth_one, "gain_one": gain_one, "shift_one": shift_one, "point_one": point_one, "gain_two": gain_two, "shift_two": shift_two, "depth_two": depth_two, "gain_three": gain_three, "shift_three": shift_three, "point_two": point_two, "gain_four": gain_four, "shift_four": shift_four}


epsilon = 1e-05

def dilated(values, weight):
    span_rows = values.shape[1]
    span_cols = values.shape[2]
    padded = jnp.pad(values, ((0, 0), (RATE, RATE), (RATE, RATE), (0, 0)))
    summed = jnp.zeros(values.shape, jnp.float32)
    for tap_row in range(3):
        for tap_col in range(3):
            window = padded[:, tap_row * RATE:tap_row * RATE + span_rows, tap_col * RATE:tap_col * RATE + span_cols, :]
            summed = summed + window.astype(jnp.float32) * weight[tap_row, tap_col].astype(jnp.float32)
    return summed

def normalize(values, gain, offset):
    pixels = values.shape[0] * values.shape[1] * values.shape[2]
    average = lax.optimization_barrier(jnp.sum(values, axis=(0, 1, 2))) / pixels
    variance = lax.optimization_barrier(jnp.sum(values * values, axis=(0, 1, 2))) / pixels - average * average
    factor = gain * lax.rsqrt(variance + epsilon)
    return jnp.maximum((values - average) * factor + offset, 0.0).astype(jnp.bfloat16)

def project(values, weight):
    shape = values.shape
    flat = values.reshape(shape[0] * shape[1] * shape[2], shape[3])
    result = jnp.dot(flat, weight, preferred_element_type=jnp.float32)
    return result.reshape(shape[0], shape[1], shape[2], weight.shape[1])

def reference(features, depth_one, gain_one, shift_one, point_one, gain_two, shift_two, depth_two, gain_three, shift_three, point_two, gain_four, shift_four):
    act_one = normalize(dilated(features, depth_one), gain_one, shift_one)
    act_two = normalize(project(act_one, point_one), gain_two, shift_two)
    act_three = normalize(dilated(act_two, depth_two), gain_three, shift_three)
    return normalize(project(act_three, point_two), gain_four, shift_four)
```

```python
import functools

import jax
import jax.numpy as jnp
from jax import lax
from jax.experimental import pallas as pl
from jax.experimental.pallas import tpu as pltpu
from jax.sharding import PartitionSpec as P

RATE = 2
EPS = 1e-05
LANES = 128
PAD = 8
CHUNK = 256
PER = CHUNK // LANES
LAG = 4
MESH = pl.DeviceIdType.MESH
F32 = jnp.float32
BF16 = jnp.bfloat16
scope = jax.named_scope


def block_rows(pixels):
    for rows in (144, 96, 48, 32, 16):
        if pixels % rows == 0:
            return rows
    return pixels


def kernel(
    n_space,
    n_batch,
    x_hbm,
    w1_hbm,
    w2_hbm,
    d1_ref,
    d2_ref,
    g1_ref,
    b1_ref,
    g2_ref,
    b2_ref,
    g3_ref,
    b3_ref,
    g4_ref,
    b4_ref,
    out,
    x_ref,
    w1_ref,
    w2_ref,
    halo1,
    edge2,
    halo2,
    xp,
    first,
    act1,
    second,
    act3,
    fourth,
    par,
    coef,
    acc,
    pa,
    pb,
    x_sem,
    w_sem,
    h1_send,
    h1_recv,
    h2_send,
    h2_recv,
    a_send,
    a_recv,
    b_send,
    b_recv,
):
    rows, cols, c_in = x_hbm.shape
    c_mid = w1_hbm.shape[1]
    c_out = w2_hbm.shape[1]
    pixels = rows * cols
    edge = RATE * cols
    total = float(pixels * n_space * n_batch)
    step = block_rows(pixels)
    k_in, k_mid, k_out = c_in // CHUNK, c_mid // CHUNK, c_out // CHUNK
    at1, at2, at3, at4 = 0, k_in, k_in + k_mid, k_in + 2 * k_mid
    n_sum = at4 + k_out
    half = n_space // 2
    n_far = n_batch * half
    sp = lax.axis_index("space")
    bt = lax.axis_index("batch")
    side = lax.rem(sp, 2)
    mine = bt * half + sp // 2
    partner = sp + 1 - 2 * side
    has_top = sp > 0
    has_bot = sp < n_space - 1
    odd = side == 1
    cross = jnp.where(odd, sp + 1, sp - 1)
    has_cross = jnp.logical_or(
        jnp.logical_and(odd, has_bot), jnp.logical_and(jnp.logical_not(odd), has_top)
    )

    def far(d):
        at = lax.rem(mine + d, n_far)
        return {"batch": at // half, "space": lax.rem(at, half) * 2 + side}

    def each_far(body):
        if n_far <= 16:
            for d in range(1, n_far):
                body(d)
        else:

            def step_far(d, carry):
                body(d)
                return carry

            lax.fori_loop(1, n_far, step_far, 0)

    spans = [(0, RATE), (rows - RATE, RATE)]
    load_edges = [
        pltpu.make_async_copy(
            x_hbm.at[pl.ds(s, n)], x_ref.at[pl.ds(s, n)], x_sem.at[q]
        )
        for q, (s, n) in enumerate(spans)
    ]

    def load_inner(c):
        block = (pl.ds(RATE, rows - 2 * RATE), slice(None), pl.ds(c * CHUNK, CHUNK))
        return pltpu.make_async_copy(x_hbm.at[block], x_ref.at[block], x_sem.at[2 + c])

    load_w1 = pltpu.make_async_copy(w1_hbm, w1_ref, w_sem.at[0])
    load_w2 = pltpu.make_async_copy(w2_hbm, w2_ref, w_sem.at[1])

    for cp in load_edges:
        cp.start()
    for c in range(k_in):
        load_inner(c).start()

    barrier = pltpu.get_barrier_semaphore()
    pl.semaphore_signal(barrier, inc=1, device_id={"space": partner}, device_id_type=MESH)

    @pl.when(has_cross)
    def _():
        pl.semaphore_signal(barrier, inc=1, device_id={"space": cross}, device_id_type=MESH)

    each_far(
        lambda d: pl.semaphore_signal(barrier, inc=1, device_id=far(d), device_id_type=MESH)
    )

    def clear(j, carry):
        for r in range(rows + 2 * RATE):
            xp[j, r, 0:PAD, :] = jnp.zeros((PAD, LANES), F32)
            xp[j, r, PAD + cols : PAD + cols + PAD, :] = jnp.zeros((PAD, LANES), F32)
        return carry

    with scope("P00clear"):
        lax.fori_loop(0, c_mid // LANES, clear, 0)
        at = 0
        for g_ref, b_ref in ((g1_ref, b1_ref), (g2_ref, b2_ref), (g3_ref, b3_ref), (g4_ref, b4_ref)):
            for c in range(g_ref.shape[0] // CHUNK):
                for q in range(PER):
                    lanes = slice(c * CHUNK + q * LANES, c * CHUNK + (q + 1) * LANES)
                    par[at, q : q + 1, :] = g_ref[lanes].reshape(1, LANES)
                    par[at, PER + q : PER + q + 1, :] = b_ref[lanes].reshape(1, LANES)
                at += 1
    with scope("P01edgewait"):
        for cp in load_edges:
            cp.wait()
    with scope("P02barrier"):
        pl.semaphore_wait(barrier, n_far + jnp.where(has_cross, 1, 0))

    def up1(p):
        lanes = pl.ds(p * CHUNK, CHUNK)
        return pltpu.make_async_remote_copy(
            src_ref=x_ref.at[pl.ds(rows - RATE, RATE), :, lanes],
            dst_ref=halo1.at[0, :, :, lanes],
            send_sem=h1_send.at[0, p],
            recv_sem=h1_recv.at[0, p],
            device_id={"space": sp + 1},
            device_id_type=MESH,
        )

    def down1(p):
        lanes = pl.ds(p * CHUNK, CHUNK)
        return pltpu.make_async_remote_copy(
            src_ref=x_ref.at[pl.ds(0, RATE), :, lanes],
            dst_ref=halo1.at[1, :, :, lanes],
            send_sem=h1_send.at[1, p],
            recv_sem=h1_recv.at[1, p],
            device_id={"space": sp - 1},
            device_id_type=MESH,
        )

    def up2(n):
        return pltpu.make_async_remote_copy(
            src_ref=edge2.at[0, n],
            dst_ref=halo2.at[0, n],
            send_sem=h2_send.at[0, n],
            recv_sem=h2_recv.at[0, n],
            device_id={"space": sp + 1},
            device_id_type=MESH,
        )

    def down2(n):
        return pltpu.make_async_remote_copy(
            src_ref=edge2.at[1, n],
            dst_ref=halo2.at[1, n],
            send_sem=h2_send.at[1, n],
            recv_sem=h2_recv.at[1, n],
            device_id={"space": sp - 1},
            device_id_type=MESH,
        )

    def send_rows(up, down, p):
        @pl.when(has_bot)
        def _():
            up(p).start()

        @pl.when(has_top)
        def _():
            down(p).start()

    def recv_rows(up, down, p):
        @pl.when(has_top)
        def _():
            up(p).wait_recv()

        @pl.when(has_bot)
        def _():
            down(p).wait_recv()

    def sent_rows(up, down, p):
        @pl.when(has_bot)
        def _():
            up(p).wait_send()

        @pl.when(has_top)
        def _():
            down(p).wait_send()

    for p in range(k_in):
        send_rows(up1, down1, p)

    for halo in (halo1, halo2):

        @pl.when(jnp.logical_not(has_top))
        def _():
            halo[0] = jnp.zeros(halo.shape[1:], BF16)

        @pl.when(jnp.logical_not(has_bot))
        def _():
            halo[1] = jnp.zeros(halo.shape[1:], BF16)

    def near_sum(i):
        return pltpu.make_async_remote_copy(
            src_ref=pa.at[i, 0],
            dst_ref=pa.at[i, 1],
            send_sem=a_send.at[i],
            recv_sem=a_recv.at[i],
            device_id={"space": partner},
            device_id_type=MESH,
        )

    def far_sum(i, d):
        return pltpu.make_async_remote_copy(
            src_ref=pb.at[i, mine],
            dst_ref=pb.at[i, mine],
            send_sem=b_send.at[i],
            recv_sem=b_recv.at[i],
            device_id=far(d),
            device_id_type=MESH,
        )

    def far_all(i):
        block = pb.at[i, pl.ds(0, n_far - 1)]
        return pltpu.make_async_remote_copy(
            src_ref=block,
            dst_ref=block,
            send_sem=b_send.at[i],
            recv_sem=b_recv.at[i],
            device_id=far(1),
            device_id_type=MESH,
        )

    def start(i):
        near_sum(i).start()

    def relay(i):
        near_sum(i).wait_recv()
        pb[i, mine] = pa[i, 0] + pa[i, 1]
        each_far(lambda d: far_sum(i, d).start())

    def finish(i):
        far_all(i).wait_recv()
        parts = [pb[i, k] for k in range(n_far)]
        while len(parts) > 1:
            parts = [a + b for a, b in zip(parts[0::2], parts[1::2])] + (
                parts[-1:] if len(parts) % 2 else []
            )
        s = parts[0] * (1.0 / total)
        mean = s[:PER]
        var = s[PER:] - mean * mean
        p = par[i]
        coef[i, 0:PER] = mean
        coef[i, PER : 2 * PER] = p[:PER] * lax.rsqrt(var + EPS)

    def normal(v, i, q):
        mean = coef[i, pl.ds(q, 1), :]
        fac = coef[i, pl.ds(PER + q, 1), :]
        return jnp.maximum((v - mean) * fac + par[i, pl.ds(PER + q, 1), :], 0.0).astype(BF16)

    def taps(d_ref, lanes):
        return [
            [d_ref[a, b : b + 1, lanes].astype(F32) for b in range(3)] for a in range(3)
        ]

    def conv_row(j, r, filt):
        y = None
        for a in range(3):
            for b in range(3):
                term = xp[j, r + RATE * a, pl.ds(PAD + RATE * (b - 1), cols), :] * filt[a][b]
                y = term if y is None else y + term
        return y

    def lanes_of(j):
        return pl.ds(pl.multiple_of(j * LANES, LANES), LANES)

    def wide_of(n):
        return pl.ds(pl.multiple_of(n * CHUNK, CHUNK), CHUNK)

    def fold(v):
        s = v[0:8]
        for k in range(1, v.shape[0] // 8):
            s = s + v[8 * k : 8 * k + 8]
        return s

    def conv_rows(j, row_list, d_ref, dst, s1, s2):
        lanes = lanes_of(j)
        filt = taps(d_ref, lanes)
        for r in row_list:
            y = conv_row(j, r, filt)
            dst[r * cols : (r + 1) * cols, lanes] = y
            s1 = s1 + fold(y)
            s2 = s2 + fold(y * y)
        return s1, s2

    def put_stats(i, q, s1, s2):
        pa[i, 0, pl.ds(q, 1), :] = jnp.sum(s1, axis=0, keepdims=True)
        pa[i, 0, pl.ds(PER + q, 1), :] = jnp.sum(s2, axis=0, keepdims=True)

    zero8 = jnp.zeros((8, LANES), F32)
    inner = list(range(RATE, rows - RATE))
    outer = list(range(RATE)) + list(range(rows - RATE, rows))

    def conv1_inner(j, carry):
        lanes = lanes_of(j)
        for r in range(rows):
            xp[j, r + RATE, PAD : PAD + cols, :] = x_ref[r, :, lanes].astype(F32)
        s1, s2 = conv_rows(j, inner, d1_ref, first, zero8, zero8)
        acc[0, j] = s1
        acc[1, j] = s2
        return carry

    for c in range(k_in):
        with scope("P03conv1inner"):
            load_inner(c).wait()
            lax.fori_loop(c * PER, (c + 1) * PER, conv1_inner, 0)
    load_w1.start()
    load_w2.start()

    def conv1_outer(i):
        def body(q, carry):
            j = i * PER + q
            lanes = lanes_of(j)
            for r in range(RATE):
                xp[j, r, PAD : PAD + cols, :] = halo1[0, r, :, lanes].astype(F32)
                xp[j, rows + RATE + r, PAD : PAD + cols, :] = halo1[1, r, :, lanes].astype(F32)
            s1, s2 = conv_rows(j, outer, d1_ref, first, acc[0, j], acc[1, j])
            put_stats(i, q, s1, s2)
            return carry

        return body

    for p in range(k_in):
        with scope("P04halo1wait"):
            recv_rows(up1, down1, p)
        with scope("P05conv1outer"):
            lax.fori_loop(0, PER, conv1_outer(p), 0)
            start(at1 + p)
        if p > 0:
            with scope("P06relay1"):
                relay(at1 + p - 1)
    with scope("P06relay1"):
        relay(at1 + k_in - 1)

    def norm_to(src, act, i, k):
        def body(q, carry):
            lanes = lanes_of(k * PER + q)
            to = lanes_of(q)
            for b in range(pixels // step):
                span = slice(b * step, (b + 1) * step)
                act[k, span, to] = normal(src[span, lanes], i, q)
            return carry

        lax.fori_loop(0, PER, body, 0)

    def tile(act, w_ref, dst, k, n, fresh):
        deep = wide_of(k)
        wide = slice(n * CHUNK, (n + 1) * CHUNK)
        y = jnp.dot(act[k], w_ref[deep, wide], preferred_element_type=F32)
        if not fresh:
            y = y + dst[:, wide]
        dst[:, wide] = y
        return y

    def tile_stats(i, y):
        s1 = fold(y)
        s2 = fold(y * y)
        for q in range(PER):
            part = slice(q * LANES, (q + 1) * LANES)
            put_stats(i, q, s1[:, part], s2[:, part])

    load_w1_waited = False
    for k in range(k_in):
        with scope("P07finish1"):
            finish(at1 + k)
        with scope("P08norm1"):
            norm_to(first, act1, at1 + k, k)
        if k == 0:
            load_w1.wait()
        with scope("P09mm1"):
            for n in range(k_mid):
                y = tile(act1, w1_ref, second, k, n, k == 0)
                if k == k_in - 1:
                    tile_stats(at2 + n, y)
                    edge2[0, n] = y[pixels - edge :].astype(BF16)
                    edge2[1, n] = y[:edge].astype(BF16)
                    start(at2 + n)
                    if n >= LAG:
                        relay(at2 + n - LAG)
                        send_rows(up2, down2, n - LAG)
    with scope("P10relay2"):
        for n in range(max(k_mid - LAG, 0), k_mid):
            relay(at2 + n)
            send_rows(up2, down2, n)

    def conv2(n):
        def body(q, carry):
            i = at2 + n
            j = n * PER + q
            lanes = lanes_of(j)
            part = lanes_of(q)
            for r in range(rows):
                v = normal(second[r * cols : (r + 1) * cols, lanes], i, q)
                xp[j, r + RATE, PAD : PAD + cols, :] = v.astype(F32)
            top = normal(halo2[0, n, :, part].astype(F32), i, q).astype(F32)
            top = jnp.where(has_top, top, 0.0)
            bot = normal(halo2[1, n, :, part].astype(F32), i, q).astype(F32)
            bot = jnp.where(has_bot, bot, 0.0)
            for r in range(RATE):
                xp[j, r, PAD : PAD + cols, :] = top[r * cols : (r + 1) * cols]
                xp[j, rows + RATE + r, PAD : PAD + cols, :] = bot[r * cols : (r + 1) * cols]
            s1, s2 = conv_rows(j, list(range(rows)), d2_ref, second, zero8, zero8)
            put_stats(at3 + n, q, s1, s2)
            return carry

        return body

    for n in range(k_mid):
        with scope("P11finish2"):
            finish(at2 + n)
        with scope("P12edgewait"):
            recv_rows(up2, down2, n)
        with scope("P13conv2"):
            lax.fori_loop(0, PER, conv2(n), 0)
            start(at3 + n)
        if n > 0:
            with scope("P14relay3"):
                relay(at3 + n - 1)
    with scope("P14relay3"):
        relay(at3 + k_mid - 1)

    for k in range(k_mid):
        with scope("P15finish3"):
            finish(at3 + k)
        with scope("P16norm3"):
            norm_to(second, act3, at3 + k, k)
        if k == 0:
            load_w2.wait()
        with scope("P17mm2"):
            for n in range(k_out):
                y = tile(act3, w2_ref, fourth, k, n, k == 0)
                if k == k_mid - 1:
                    tile_stats(at4 + n, y)
                    start(at4 + n)
                    if n >= LAG:
                        relay(at4 + n - LAG)
    with scope("P18relay4"):
        for n in range(max(k_out - LAG, 0), k_out):
            relay(at4 + n)

    def last(n, carry):
        i = at4 + n
        finish(i)
        for q in range(PER):
            lanes = lanes_of(n * PER + q)
            for b in range(pixels // step):
                span = slice(b * step, (b + 1) * step)
                out[span, lanes] = normal(fourth[span, lanes], i, q)
        return carry

    with scope("P19last"):
        for n in range(k_out):
            last(n, 0)

    with scope("P20drain"):
        for p in range(k_in):
            sent_rows(up1, down1, p)
        for n in range(k_mid):
            sent_rows(up2, down2, n)
        for i in range(n_sum):
            near_sum(i).wait_send()
            far_all(i).wait_send()


def per_device(
    features,
    depth_one,
    gain_one,
    shift_one,
    point_one,
    gain_two,
    shift_two,
    depth_two,
    gain_three,
    shift_three,
    point_two,
    gain_four,
    shift_four,
):
    samples, span_rows, cols, c_in = features.shape
    rows = samples * span_rows
    assert samples == 1
    c_mid = point_one.shape[1]
    c_out = point_two.shape[1]
    pixels = rows * cols
    n_space = lax.axis_size("space")
    n_batch = lax.axis_size("batch")
    k_in, k_mid, k_out = c_in // CHUNK, c_mid // CHUNK, c_out // CHUNK
    n_sum = k_in + 2 * k_mid + k_out
    n_far = n_batch * n_space // 2
    any_spec = pl.BlockSpec(memory_space=pl.ANY)
    vmem = pl.BlockSpec(memory_space=pltpu.VMEM)
    edge = RATE * cols
    DMA = pltpu.SemaphoreType.DMA
    out = pl.pallas_call(
        functools.partial(kernel, n_space, n_batch),
        out_shape=pltpu.VMEM((pixels, c_out), BF16),
        in_specs=[any_spec] * 3 + [vmem] * 10,
        out_specs=vmem,
        scratch_shapes=[
            pltpu.VMEM((rows, cols, c_in), BF16),
            pltpu.VMEM((c_in, c_mid), BF16),
            pltpu.VMEM((c_mid, c_out), BF16),
            pltpu.VMEM((2, RATE, cols, c_in), BF16),
            pltpu.VMEM((2, k_mid, edge, CHUNK), BF16),
            pltpu.VMEM((2, k_mid, edge, CHUNK), BF16),
            pltpu.VMEM((c_mid // LANES, rows + 2 * RATE, cols + 2 * PAD, LANES), F32),
            pltpu.VMEM((pixels, c_in), F32),
            pltpu.VMEM((k_in, pixels, CHUNK), BF16),
            pltpu.VMEM((pixels, c_mid), F32),
            pltpu.VMEM((k_mid, pixels, CHUNK), BF16),
            pltpu.VMEM((pixels, c_out), F32),
            pltpu.VMEM((n_sum, 2 * PER, LANES), F32),
            pltpu.VMEM((n_sum, 2 * PER, LANES), F32),
            pltpu.VMEM((2, c_in // LANES, 8, LANES), F32),
            pltpu.VMEM((n_sum, 2, 2 * PER, LANES), F32),
            pltpu.VMEM((n_sum, n_far, 2 * PER, LANES), F32),
            DMA((2 + k_in,)),
            DMA((2,)),
            DMA((2, k_in)),
            DMA((2, k_in)),
            DMA((2, k_mid)),
            DMA((2, k_mid)),
            DMA((n_sum,)),
            DMA((n_sum,)),
            DMA((n_sum,)),
            DMA((n_sum,)),
        ],
        compiler_params=pltpu.CompilerParams(
            collective_id=0, has_side_effects=True, vmem_limit_bytes=56 * 1024 * 1024
        ),
        name="exit_block",
    )(
        features.reshape(rows, cols, c_in),
        point_one,
        point_two,
        depth_one,
        depth_two,
        gain_one,
        shift_one,
        gain_two,
        shift_two,
        gain_three,
        shift_three,
        gain_four,
        shift_four,
    )
    return out.reshape(samples, span_rows, cols, c_out)


def solution(mesh):
    return jax.shard_map(
        per_device,
        mesh=mesh,
        in_specs=(P("batch", "space", None, None),) + (P(),) * 12,
        out_specs=P("batch", "space", None, None),
        check_vma=False,
    )
```

```python
import functools

import jax
import jax.numpy as jnp
from jax import lax
from jax.experimental import pallas as pl
from jax.experimental.pallas import tpu as pltpu
from jax.sharding import PartitionSpec as P

RATE = 2
EPS = 1e-05
LANES = 128
PAD = 8
CHUNK = 256
PER = CHUNK // LANES
WIDE = 1
TAIL = 2
SLACK = 3
DIRECT = 32
ENDS = 2
MESH = pl.DeviceIdType.MESH
F32 = jnp.float32
BF16 = jnp.bfloat16
scope = jax.named_scope


def block_rows(pixels):
    for rows in (144, 96, 48, 32, 16):
        if pixels % rows == 0:
            return rows
    return pixels


def lines_of(n_batch):
    n_y = 1
    while 8 * n_y * n_y <= n_batch and n_batch % (2 * n_y) == 0:
        n_y *= 2
    return n_y


def kernel(
    n_space,
    n_batch,
    x_hbm,
    w1_hbm,
    w2_hbm,
    d1_hbm,
    d2_hbm,
    g1_hbm,
    b1_hbm,
    g2_hbm,
    b2_hbm,
    g3_hbm,
    b3_hbm,
    g4_hbm,
    b4_hbm,
    out,
    d1_ref,
    d2_ref,
    g1_ref,
    b1_ref,
    g2_ref,
    b2_ref,
    g3_ref,
    b3_ref,
    g4_ref,
    b4_ref,
    x_ref,
    w1_ref,
    w2_ref,
    halo1,
    edge2,
    halo2,
    xp,
    first,
    act1,
    second,
    act3,
    fourth,
    par,
    coef,
    acc,
    pa,
    pb,
    x_sem,
    w_sem,
    p_sem,
    h1_send,
    h1_recv,
    h2_send,
    h2_recv,
    a_send,
    a_recv,
    b_send,
    b_recv,
    rise,
    fall,
):
    rows, cols, c_in = x_hbm.shape
    c_mid = w1_hbm.shape[1]
    c_out = w2_hbm.shape[1]
    pixels = rows * cols
    edge = RATE * cols
    total = float(pixels * n_space * n_batch)
    step = block_rows(pixels)
    k_in, k_mid, k_out = c_in // CHUNK, c_mid // CHUNK, c_out // CHUNK
    at1, at2, at3, at4 = 0, k_in, k_in + k_mid, k_in + 2 * k_mid
    n_sum = at4 + k_out
    half = n_space // 2
    n_far = n_batch * half
    sp = lax.axis_index("space")
    bt = lax.axis_index("batch")
    side = lax.rem(sp, 2)
    mine = bt * half + sp // 2
    partner = sp + 1 - 2 * side
    has_top = sp > 0
    has_bot = sp < n_space - 1
    n_all = n_batch * n_space
    self = bt * n_space + sp

    def other(d):
        at = lax.rem(self + d, n_all)
        return {"batch": at // n_space, "space": lax.rem(at, n_space)}

    def far(d):
        at = lax.rem(mine + d, n_far)
        return {"batch": at // half, "space": lax.rem(at, half) * 2 + side}

    n_y = lines_of(n_batch)
    n_z = n_batch // n_y
    n_plane = n_y * n_space
    pos_z = bt // n_y
    pos_plane = lax.rem(bt, n_y) * n_space + sp

    def plane(d):
        at = lax.rem(pos_plane + d, n_plane)
        return {"batch": pos_z * n_y + at // n_space, "space": lax.rem(at, n_space)}

    def line(d):
        return {"batch": lax.rem(pos_z + d, n_z) * n_y + lax.rem(bt, n_y), "space": sp}

    def each(count, body):
        if count <= 32:
            for d in range(1, count):
                body(d)
        else:

            def step_one(d, carry):
                body(d)
                return carry

            lax.fori_loop(1, count, step_one, 0)

    def each_other(body):
        each(n_all, body)

    spans = [(0, RATE), (rows - RATE, RATE)]
    load_edges = [
        pltpu.make_async_copy(
            x_hbm.at[pl.ds(s, n)], x_ref.at[pl.ds(s, n)], x_sem.at[q]
        )
        for q, (s, n) in enumerate(spans)
    ]

    def load_inner(c):
        block = (pl.ds(RATE, rows - 2 * RATE), slice(None), pl.ds(c * CHUNK, CHUNK))
        return pltpu.make_async_copy(x_hbm.at[block], x_ref.at[block], x_sem.at[2 + c])

    load_w1 = pltpu.make_async_copy(w1_hbm, w1_ref, w_sem.at[0])
    load_w2 = pltpu.make_async_copy(w2_hbm, w2_ref, w_sem.at[1])

    small = (d1_hbm, d2_hbm, g1_hbm, b1_hbm, g2_hbm, b2_hbm, g3_hbm, b3_hbm, g4_hbm, b4_hbm)
    small_to = (d1_ref, d2_ref, g1_ref, b1_ref, g2_ref, b2_ref, g3_ref, b3_ref, g4_ref, b4_ref)
    load_small = [
        pltpu.make_async_copy(a, b, p_sem.at[q]) for q, (a, b) in enumerate(zip(small, small_to))
    ]
    for cp in load_edges:
        cp.start()
    for c in range(k_in):
        load_inner(c).start()
    for cp in load_small:
        cp.start()

    below, above = pos_z > 0, pos_z < n_z - 1
    inside = jnp.logical_and(below, above)

    def tell(sem, device):
        pl.semaphore_signal(sem, inc=1, device_id=device, device_id_type=MESH)

    def tell_if(condition, sem, step_z):
        @pl.when(condition)
        def _():
            tell(sem, {"batch": bt + step_z * n_y})

    def wait_if(condition, sem):
        @pl.when(condition)
        def _():
            pl.semaphore_wait(sem, 1)

    barrier = pltpu.get_barrier_semaphore()
    each(n_plane, lambda d: tell(barrier, plane(d)))
    tell_if(below, barrier, -1)
    tell_if(above, barrier, 1)
    near = n_plane - 1 + jnp.where(below, 1, 0) + jnp.where(above, 1, 0)

    rise_at = jnp.minimum(pos_z - 1, k_in - 2)
    fall_at = jnp.where(pos_z == n_z - 2, 1, k_in - 1)

    def meet(c):
        now = rise_at == c
        wait_if(jnp.logical_and(below, now), rise)
        tell_if(jnp.logical_and(inside, now), rise, 1)
        now = fall_at == c
        wait_if(jnp.logical_and(above, now), fall)
        tell_if(jnp.logical_and(inside, now), fall, -1)

    def clear(j, carry):
        for r in range(rows + 2 * RATE):
            xp[j, r, 0:PAD, :] = jnp.zeros((PAD, LANES), F32)
            xp[j, r, PAD + cols : PAD + cols + PAD, :] = jnp.zeros((PAD, LANES), F32)
        return carry

    with scope("P00clear"):
        lax.fori_loop(0, c_mid // LANES, clear, 0)
    with scope("P01edgewait"):
        for cp in load_edges:
            cp.wait()
    with scope("P02barrier"):
        pl.semaphore_wait(barrier, near)
        tell_if(jnp.logical_and(above, jnp.logical_not(below)), rise, 1)
        tell_if(jnp.logical_and(below, jnp.logical_not(above)), fall, -1)

    def up1(p):
        lanes = pl.ds(p * CHUNK, CHUNK)
        return pltpu.make_async_remote_copy(
            src_ref=x_ref.at[pl.ds(rows - RATE, RATE), :, lanes],
            dst_ref=halo1.at[0, :, :, lanes],
            send_sem=h1_send.at[0, p],
            recv_sem=h1_recv.at[0, p],
            device_id={"space": sp + 1},
            device_id_type=MESH,
        )

    def down1(p):
        lanes = pl.ds(p * CHUNK, CHUNK)
        return pltpu.make_async_remote_copy(
            src_ref=x_ref.at[pl.ds(0, RATE), :, lanes],
            dst_ref=halo1.at[1, :, :, lanes],
            send_sem=h1_send.at[1, p],
            recv_sem=h1_recv.at[1, p],
            device_id={"space": sp - 1},
            device_id_type=MESH,
        )

    def up2(n):
        return pltpu.make_async_remote_copy(
            src_ref=edge2.at[0, n],
            dst_ref=halo2.at[0, n],
            send_sem=h2_send.at[0, n],
            recv_sem=h2_recv.at[0, n],
            device_id={"space": sp + 1},
            device_id_type=MESH,
        )

    def down2(n):
        return pltpu.make_async_remote_copy(
            src_ref=edge2.at[1, n],
            dst_ref=halo2.at[1, n],
            send_sem=h2_send.at[1, n],
            recv_sem=h2_recv.at[1, n],
            device_id={"space": sp - 1},
            device_id_type=MESH,
        )

    def send_rows(up, down, p):
        @pl.when(has_bot)
        def _():
            up(p).start()

        @pl.when(has_top)
        def _():
            down(p).start()

    def recv_rows(up, down, p):
        @pl.when(has_top)
        def _():
            up(p).wait_recv()

        @pl.when(has_bot)
        def _():
            down(p).wait_recv()

    def sent_rows(up, down, p):
        @pl.when(has_bot)
        def _():
            up(p).wait_send()

        @pl.when(has_top)
        def _():
            down(p).wait_send()

    for p in range(k_in):
        send_rows(up1, down1, p)

    for halo in (halo1, halo2):

        @pl.when(jnp.logical_not(has_top))
        def _():
            halo[0] = jnp.zeros(halo.shape[1:], BF16)

        @pl.when(jnp.logical_not(has_bot))
        def _():
            halo[1] = jnp.zeros(halo.shape[1:], BF16)

    def kind(i):
        if n_all > DIRECT:
            return "grid"
        if i in (at1, at2, at3, at3 + k_mid - 1):
            return "one"
        if at4 <= i < n_sum - ENDS or at2 + SLACK <= i < at3:
            return "grid"
        return "pair"

    def home(i):
        how = kind(i)
        if how == "one":
            return pb.at[i, self]
        return pa.at[i, pos_plane] if how == "grid" else pa.at[i, side]

    def hop(buf, i, slot, send, recv, device):
        return pltpu.make_async_remote_copy(
            src_ref=buf.at[i, slot],
            dst_ref=buf.at[i, slot],
            send_sem=send.at[i],
            recv_sem=recv.at[i],
            device_id=device,
            device_id_type=MESH,
        )

    def bulk(buf, i, count, send, recv, device):
        block = buf.at[i, pl.ds(0, count)]
        return pltpu.make_async_remote_copy(
            src_ref=block,
            dst_ref=block,
            send_sem=send.at[i],
            recv_sem=recv.at[i],
            device_id=device,
            device_id_type=MESH,
        )

    def near_all(i):
        if kind(i) == "grid":
            return bulk(pa, i, n_plane - 1, a_send, a_recv, plane(1))
        return bulk(pa, i, 1, a_send, a_recv, {"space": partner})

    def far_count(i):
        return {"one": n_all, "pair": n_far, "grid": n_z}[kind(i)]

    def far_all(i):
        device = {"one": other, "pair": far, "grid": line}[kind(i)](1)
        return bulk(pb, i, far_count(i) - 1, b_send, b_recv, device)

    def start(i):
        how = kind(i)
        if how == "one":
            each_other(lambda d: hop(pb, i, self, b_send, b_recv, other(d)).start())
        elif how == "grid":
            each(n_plane, lambda d: hop(pa, i, pos_plane, a_send, a_recv, plane(d)).start())
        else:
            hop(pa, i, side, a_send, a_recv, {"space": partner}).start()

    def relay(i):
        how = kind(i)
        if how == "one":
            return
        near_all(i).wait_recv()
        if how == "grid":
            s = pa[i, 0]
            for k in range(1, n_plane):
                s = s + pa[i, k]
            pb[i, pos_z] = s
            each(n_z, lambda d: hop(pb, i, pos_z, b_send, b_recv, line(d)).start())
        else:
            pb[i, mine] = pa[i, 0] + pa[i, 1]
            each(n_far, lambda d: hop(pb, i, mine, b_send, b_recv, far(d)).start())

    def finish(i):
        far_all(i).wait_recv()
        parts = [pb[i, k] for k in range(far_count(i))]
        while len(parts) > 1:
            parts = [a + b for a, b in zip(parts[0::2], parts[1::2])] + (
                parts[-1:] if len(parts) % 2 else []
            )
        s = parts[0] * (1.0 / total)
        mean = s[:PER]
        var = s[PER:] - mean * mean
        p = par[i]
        fac = p[:PER] * lax.rsqrt(var + EPS)
        coef[i, 0:PER] = fac
        coef[i, PER : 2 * PER] = p[PER:] - mean * fac

    def normal(v, i, q):
        return jnp.maximum(v * coef[i, pl.ds(q, 1), :] + coef[i, pl.ds(PER + q, 1), :], 0.0)

    def taps(d_ref, lanes):
        return [
            [d_ref[a, b : b + 1, lanes].astype(F32) for b in range(3)] for a in range(3)
        ]

    def conv_row(j, r, filt):
        y = None
        for a in range(3):
            for b in range(3):
                term = xp[j, r + RATE * a, pl.ds(PAD + RATE * (b - 1), cols), :] * filt[a][b]
                y = term if y is None else y + term
        return y

    def lanes_of(j):
        if isinstance(j, int):
            return slice(j * LANES, (j + 1) * LANES)
        return pl.ds(pl.multiple_of(j * LANES, LANES), LANES)

    def wide_of(n):
        if isinstance(n, int):
            return slice(n * CHUNK, (n + 1) * CHUNK)
        return pl.ds(pl.multiple_of(n * CHUNK, CHUNK), CHUNK)

    def fold(v):
        s = v[0:8]
        for k in range(1, v.shape[0] // 8):
            s = s + v[8 * k : 8 * k + 8]
        return s

    def conv_rows(j, row_list, d_ref, dst, s1, s2):
        lanes = lanes_of(j)
        filt = taps(d_ref, lanes)
        for r in row_list:
            y = conv_row(j, r, filt)
            dst[r * cols : (r + 1) * cols, lanes] = y
            s1 = s1 + fold(y)
            s2 = s2 + fold(y * y)
        return s1, s2

    def put_stats(i, q, s1, s2):
        to = home(i)
        to[pl.ds(q, 1), :] = jnp.sum(s1, axis=0, keepdims=True)
        to[pl.ds(PER + q, 1), :] = jnp.sum(s2, axis=0, keepdims=True)

    zero8 = jnp.zeros((8, LANES), F32)
    inner = list(range(RATE, rows - RATE))
    outer = list(range(RATE)) + list(range(rows - RATE, rows))

    def conv1_inner(j, carry):
        lanes = lanes_of(j)
        for r in range(rows):
            xp[j, r + RATE, PAD : PAD + cols, :] = x_ref[r, :, lanes].astype(F32)
        s1, s2 = conv_rows(j, inner, d1_ref, first, zero8, zero8)
        acc[0, j] = s1
        acc[1, j] = s2
        return carry

    for cp in load_small[:2]:
        cp.wait()
    for c in range(k_in):
        with scope("P03conv1inner"):
            load_inner(c).wait()
            lax.fori_loop(c * PER, (c + 1) * PER, conv1_inner, 0)
        with scope("P03meet"):
            meet(c)
    load_w1.start()
    load_w2.start()
    for cp in load_small[2:]:
        cp.wait()
    at = 0
    for g_ref, b_ref in ((g1_ref, b1_ref), (g2_ref, b2_ref), (g3_ref, b3_ref), (g4_ref, b4_ref)):
        for c in range(g_ref.shape[0] // CHUNK):
            for q in range(PER):
                lanes = slice(c * CHUNK + q * LANES, c * CHUNK + (q + 1) * LANES)
                par[at, q : q + 1, :] = g_ref[lanes].reshape(1, LANES)
                par[at, PER + q : PER + q + 1, :] = b_ref[lanes].reshape(1, LANES)
            at += 1

    def conv1_outer(i):
        def body(q, carry):
            j = i * PER + q
            lanes = lanes_of(j)
            for r in range(RATE):
                xp[j, r, PAD : PAD + cols, :] = halo1[0, r, :, lanes].astype(F32)
                xp[j, rows + RATE + r, PAD : PAD + cols, :] = halo1[1, r, :, lanes].astype(F32)
            s1, s2 = conv_rows(j, outer, d1_ref, first, acc[0, j], acc[1, j])
            put_stats(i, q, s1, s2)
            return carry

        return body

    for p in range(k_in):
        with scope("P04halo1wait"):
            recv_rows(up1, down1, p)
        with scope("P05conv1outer"):
            lax.fori_loop(0, PER, conv1_outer(p), 0)
            start(at1 + p)
        if p > 0:
            with scope("P06relay1"):
                relay(at1 + p - 1)
    with scope("P06relay1"):
        relay(at1 + k_in - 1)

    def norm_to(src, act, i, k):
        for b in range(pixels // step):
            span = slice(b * step, (b + 1) * step)
            for q in range(PER):
                lanes = lanes_of(k * PER + q)
                act[k, span, lanes_of(q)] = normal(src[span, lanes], i, q).astype(BF16)

    def tile(act, w_ref, dst, ks, n0, n1, fresh):
        wide = slice(n0 * CHUNK, n1 * CHUNK)
        y = None if fresh else dst[:, wide]
        for k in ks:
            z = jnp.dot(act[k], w_ref[wide_of(k), wide], preferred_element_type=F32)
            y = z if y is None else y + z
        dst[:, wide] = y
        return y

    def pairs(count):
        return [(n, min(n + WIDE, count)) for n in range(0, count, WIDE)]

    def tile_sums(i, s1, s2):
        for q in range(PER):
            part = slice(q * LANES, (q + 1) * LANES)
            put_stats(i, q, s1[:, part], s2[:, part])
        start(i)

    def groups(count, first_ones):
        at = 0
        for size in first_ones:
            if at + size < count:
                yield list(range(at, at + size))
                at += size
        yield list(range(at, count))

    for k in range(k_in):
        with scope("P07finish1"):
            finish(at1 + k)
        with scope("P08norm1"):
            norm_to(first, act1, at1 + k, k)
        if k == 0:
            load_w1.wait()
        with scope("P09mm1"):
            if k < k_in - 1:
                for n0, n1 in pairs(k_mid):
                    tile(act1, w1_ref, second, (k,), n0, n1, k == 0)
                continue
            for group in groups(k_mid, (1, 2)):
                sums = []
                for n in group:
                    y = tile(act1, w1_ref, second, (k,), n, n + 1, k == 0)
                    sums.append((at2 + n, fold(y), fold(y * y)))
                    edge2[0, n] = y[pixels - edge :].astype(BF16)
                    edge2[1, n] = y[:edge].astype(BF16)
                for s in sums:
                    tile_sums(*s)
    with scope("P10relay2"):
        for n in range(min(SLACK, k_mid)):
            relay(at2 + n)
            send_rows(up2, down2, n)
        for n in range(SLACK, k_mid):
            send_rows(up2, down2, n)

    def conv2(n):
        def body(q, carry):
            i = at2 + n
            j = n * PER + q
            lanes = lanes_of(j)
            part = lanes_of(q)
            for r in range(rows):
                v = normal(second[r * cols : (r + 1) * cols, lanes], i, q)
                xp[j, r + RATE, PAD : PAD + cols, :] = v
            top = normal(halo2[0, n, :, part].astype(F32), i, q)
            top = jnp.where(has_top, top, 0.0)
            bot = normal(halo2[1, n, :, part].astype(F32), i, q)
            bot = jnp.where(has_bot, bot, 0.0)
            for r in range(RATE):
                xp[j, r, PAD : PAD + cols, :] = top[r * cols : (r + 1) * cols]
                xp[j, rows + RATE + r, PAD : PAD + cols, :] = bot[r * cols : (r + 1) * cols]
            s1, s2 = conv_rows(j, list(range(rows)), d2_ref, second, zero8, zero8)
            put_stats(at3 + n, q, s1, s2)
            return carry

        return body

    for n in range(k_mid):
        with scope("P11finish2"):
            finish(at2 + n)
        with scope("P12edgewait"):
            recv_rows(up2, down2, n)
        with scope("P13conv2"):
            lax.fori_loop(0, PER, conv2(n), 0)
            start(at3 + n)
        with scope("P14relay3"):
            if n > 0:
                relay(at3 + n - 1)
            else:
                for late in range(SLACK, k_mid):
                    relay(at2 + late)
    with scope("P14relay3"):
        relay(at3 + k_mid - 1)

    for k in range(k_mid):
        with scope("P15finish3"):
            finish(at3 + k)
        with scope("P16norm3"):
            norm_to(second, act3, at3 + k, k)
        if k == 0:
            load_w2.wait()
        with scope("P17mm2"):
            if k < k_mid - TAIL:
                for n0, n1 in pairs(k_out):
                    tile(act3, w2_ref, fourth, (k,), n0, n1, k == 0)
            if k == k_mid - 1:
                last_ks = tuple(range(max(k_mid - TAIL, 0), k_mid))
                for group in groups(k_out, (3, 3)):
                    sums = []
                    for n in group:
                        y = tile(act3, w2_ref, fourth, last_ks, n, n + 1, last_ks[0] == 0)
                        sums.append((at4 + n, fold(y), fold(y * y)))
                    for s in sums:
                        tile_sums(*s)
    with scope("P18relay4"):
        for n in list(range(k_out - ENDS, k_out)) + list(range(k_out - ENDS)):
            relay(at4 + n)

    def last(n, carry):
        i = at4 + n
        finish(i)
        for q in range(PER):
            lanes = lanes_of(n * PER + q)
            for b in range(pixels // step):
                span = slice(b * step, (b + 1) * step)
                out[span, lanes] = normal(fourth[span, lanes], i, q).astype(BF16)
        return carry

    with scope("P19last"):
        for n in list(range(3)) + list(range(k_out - ENDS, k_out)) + list(range(3, k_out - ENDS)):
            last(n, 0)

    with scope("P20drain"):
        for p in range(k_in):
            sent_rows(up1, down1, p)
        for n in range(k_mid):
            sent_rows(up2, down2, n)
        for i in range(n_sum):
            if kind(i) != "one":
                near_all(i).wait_send()
            far_all(i).wait_send()


def per_device(
    features,
    depth_one,
    gain_one,
    shift_one,
    point_one,
    gain_two,
    shift_two,
    depth_two,
    gain_three,
    shift_three,
    point_two,
    gain_four,
    shift_four,
):
    samples, span_rows, cols, c_in = features.shape
    rows = samples * span_rows
    assert samples == 1
    c_mid = point_one.shape[1]
    c_out = point_two.shape[1]
    pixels = rows * cols
    n_space = lax.axis_size("space")
    n_batch = lax.axis_size("batch")
    k_in, k_mid, k_out = c_in // CHUNK, c_mid // CHUNK, c_out // CHUNK
    n_sum = k_in + 2 * k_mid + k_out
    n_all = n_batch * n_space
    slots = n_all if n_all <= DIRECT else n_batch // lines_of(n_batch)
    any_spec = pl.BlockSpec(memory_space=pl.ANY)
    vmem = pl.BlockSpec(memory_space=pltpu.VMEM)
    edge = RATE * cols
    DMA = pltpu.SemaphoreType.DMA
    out = pl.pallas_call(
        functools.partial(kernel, n_space, n_batch),
        out_shape=pltpu.VMEM((pixels, c_out), BF16),
        in_specs=[any_spec] * 13,
        out_specs=vmem,
        scratch_shapes=[
            pltpu.VMEM(depth_one.shape, BF16),
            pltpu.VMEM(depth_two.shape, BF16),
        ]
        + [pltpu.VMEM((c,), F32) for c in (c_in, c_in, c_mid, c_mid, c_mid, c_mid, c_out, c_out)]
        + [
            pltpu.VMEM((rows, cols, c_in), BF16),
            pltpu.VMEM((c_in, c_mid), BF16),
            pltpu.VMEM((c_mid, c_out), BF16),
            pltpu.VMEM((2, RATE, cols, c_in), BF16),
            pltpu.VMEM((2, k_mid, edge, CHUNK), BF16),
            pltpu.VMEM((2, k_mid, edge, CHUNK), BF16),
            pltpu.VMEM((c_mid // LANES, rows + 2 * RATE, cols + 2 * PAD, LANES), F32),
            pltpu.VMEM((pixels, c_in), F32),
            pltpu.VMEM((k_in, pixels, CHUNK), BF16),
            pltpu.VMEM((pixels, c_mid), F32),
            pltpu.VMEM((k_mid, pixels, CHUNK), BF16),
            pltpu.VMEM((pixels, c_out), F32),
            pltpu.VMEM((n_sum, 2 * PER, LANES), F32),
            pltpu.VMEM((n_sum, 2 * PER, LANES), F32),
            pltpu.VMEM((2, c_in // LANES, 8, LANES), F32),
            pltpu.VMEM((n_sum, lines_of(n_batch) * n_space, 2 * PER, LANES), F32),
            pltpu.VMEM((n_sum, slots, 2 * PER, LANES), F32),
            DMA((2 + k_in,)),
            DMA((2,)),
            DMA((10,)),
            DMA((2, k_in)),
            DMA((2, k_in)),
            DMA((2, k_mid)),
            DMA((2, k_mid)),
            DMA((n_sum,)),
            DMA((n_sum,)),
            DMA((n_sum,)),
            DMA((n_sum,)),
            pltpu.SemaphoreType.REGULAR,
            pltpu.SemaphoreType.REGULAR,
        ],
        compiler_params=pltpu.CompilerParams(
            collective_id=0, has_side_effects=True, vmem_limit_bytes=56 * 1024 * 1024
        ),
        name="exit_block",
    )(
        features.reshape(rows, cols, c_in),
        point_one,
        point_two,
        depth_one,
        depth_two,
        gain_one,
        shift_one,
        gain_two,
        shift_two,
        gain_three,
        shift_three,
        gain_four,
        shift_four,
    )
    return out.reshape(samples, span_rows, cols, c_out)


def solution(mesh):
    return jax.shard_map(
        per_device,
        mesh=mesh,
        in_specs=(P("batch", "space", None, None),) + (P(),) * 12,
        out_specs=P("batch", "space", None, None),
        check_vma=False,
    )
```

```python
import functools

import jax
import jax.numpy as jnp
from jax import lax
from jax.experimental import pallas as pl
from jax.experimental.pallas import tpu as pltpu
from jax.sharding import PartitionSpec as P

RATE = 2
EPS = 1e-05
LANES = 128
PAD = 8
CHUNK = 256
PER = CHUNK // LANES
WIDE = 1
TAIL = 2
SLACK = 3
DIRECT = 32
ENDS = 4
MESH = pl.DeviceIdType.MESH
F32 = jnp.float32
BF16 = jnp.bfloat16
scope = jax.named_scope


def block_rows(pixels):
    for rows in (144, 96, 48, 32, 16):
        if pixels % rows == 0:
            return rows
    return pixels


def lines_of(n_batch):
    n_y = 1
    while 8 * n_y * n_y <= n_batch and n_batch % (2 * n_y) == 0:
        n_y *= 2
    return n_y


def kernel(
    n_space,
    n_batch,
    x_hbm,
    w1_hbm,
    w2_hbm,
    d1_hbm,
    d2_hbm,
    g1_hbm,
    b1_hbm,
    g2_hbm,
    b2_hbm,
    g3_hbm,
    b3_hbm,
    g4_hbm,
    b4_hbm,
    out,
    d1_ref,
    d2_ref,
    g1_ref,
    b1_ref,
    g2_ref,
    b2_ref,
    g3_ref,
    b3_ref,
    g4_ref,
    b4_ref,
    x_ref,
    w1_ref,
    w2_ref,
    halo1,
    edge2,
    halo2,
    xp,
    first,
    act1,
    second,
    act3,
    fourth,
    par,
    coef,
    acc,
    pa,
    pb,
    x_sem,
    w_sem,
    p_sem,
    h1_send,
    h1_recv,
    h2_send,
    h2_recv,
    a_send,
    a_recv,
    b_send,
    b_recv,
    rise,
    fall,
):
    rows, cols, c_in = x_hbm.shape
    c_mid = w1_hbm.shape[1]
    c_out = w2_hbm.shape[1]
    pixels = rows * cols
    edge = RATE * cols
    total = float(pixels * n_space * n_batch)
    step = block_rows(pixels)
    k_in, k_mid, k_out = c_in // CHUNK, c_mid // CHUNK, c_out // CHUNK
    at1, at2, at3, at4 = 0, k_in, k_in + k_mid, k_in + 2 * k_mid
    n_sum = at4 + k_out
    half = n_space // 2
    n_far = n_batch * half
    sp = lax.axis_index("space")
    bt = lax.axis_index("batch")
    side = lax.rem(sp, 2)
    mine = bt * half + sp // 2
    partner = sp + 1 - 2 * side
    has_top = sp > 0
    has_bot = sp < n_space - 1
    n_all = n_batch * n_space
    self = bt * n_space + sp

    def other(d):
        at = lax.rem(self + d, n_all)
        return {"batch": at // n_space, "space": lax.rem(at, n_space)}

    def far(d):
        at = lax.rem(mine + d, n_far)
        return {"batch": at // half, "space": lax.rem(at, half) * 2 + side}

    n_y = lines_of(n_batch)
    n_z = n_batch // n_y
    n_plane = n_y * n_space
    pos_z = bt // n_y
    pos_plane = lax.rem(bt, n_y) * n_space + sp

    def plane(d):
        at = lax.rem(pos_plane + d, n_plane)
        return {"batch": pos_z * n_y + at // n_space, "space": lax.rem(at, n_space)}

    def line(d):
        return {"batch": lax.rem(pos_z + d, n_z) * n_y + lax.rem(bt, n_y), "space": sp}

    def each(count, body):
        if count <= 32:
            for d in range(1, count):
                body(d)
        else:

            def step_one(d, carry):
                body(d)
                return carry

            lax.fori_loop(1, count, step_one, 0)

    def each_other(body):
        each(n_all, body)

    spans = [(0, RATE), (rows - RATE, RATE)]
    load_edges = [
        pltpu.make_async_copy(
            x_hbm.at[pl.ds(s, n)], x_ref.at[pl.ds(s, n)], x_sem.at[q]
        )
        for q, (s, n) in enumerate(spans)
    ]

    def load_inner(c):
        block = (pl.ds(RATE, rows - 2 * RATE), slice(None), pl.ds(c * CHUNK, CHUNK))
        return pltpu.make_async_copy(x_hbm.at[block], x_ref.at[block], x_sem.at[2 + c])

    load_w1 = pltpu.make_async_copy(w1_hbm, w1_ref, w_sem.at[0])
    load_w2 = pltpu.make_async_copy(w2_hbm, w2_ref, w_sem.at[1])

    small = (d1_hbm, d2_hbm, g1_hbm, b1_hbm, g2_hbm, b2_hbm, g3_hbm, b3_hbm, g4_hbm, b4_hbm)
    small_to = (d1_ref, d2_ref, g1_ref, b1_ref, g2_ref, b2_ref, g3_ref, b3_ref, g4_ref, b4_ref)
    load_small = [
        pltpu.make_async_copy(a, b, p_sem.at[q]) for q, (a, b) in enumerate(zip(small, small_to))
    ]
    for cp in load_edges:
        cp.start()
    for c in range(k_in):
        load_inner(c).start()
    for cp in load_small:
        cp.start()

    below, above = pos_z > 0, pos_z < n_z - 1
    inside = jnp.logical_and(below, above)

    def tell(sem, device):
        pl.semaphore_signal(sem, inc=1, device_id=device, device_id_type=MESH)

    def tell_if(condition, sem, step_z):
        @pl.when(condition)
        def _():
            tell(sem, {"batch": bt + step_z * n_y})

    def wait_if(condition, sem):
        @pl.when(condition)
        def _():
            pl.semaphore_wait(sem, 1)

    barrier = pltpu.get_barrier_semaphore()
    each(n_plane, lambda d: tell(barrier, plane(d)))
    tell_if(below, barrier, -1)
    tell_if(above, barrier, 1)
    near = n_plane - 1 + jnp.where(below, 1, 0) + jnp.where(above, 1, 0)

    rise_at = jnp.minimum(pos_z - 1, k_in - 2)
    fall_at = jnp.where(pos_z == n_z - 2, 1, k_in - 1)

    def meet(c):
        now = rise_at == c
        wait_if(jnp.logical_and(below, now), rise)
        tell_if(jnp.logical_and(inside, now), rise, 1)
        now = fall_at == c
        wait_if(jnp.logical_and(above, now), fall)
        tell_if(jnp.logical_and(inside, now), fall, -1)

    def clear(j, carry):
        for r in range(rows + 2 * RATE):
            xp[j, r, 0:PAD, :] = jnp.zeros((PAD, LANES), F32)
            xp[j, r, PAD + cols : PAD + cols + PAD, :] = jnp.zeros((PAD, LANES), F32)
        return carry

    with scope("P00clear"):
        lax.fori_loop(0, c_mid // LANES, clear, 0)
    with scope("P01edgewait"):
        for cp in load_edges:
            cp.wait()
    with scope("P02barrier"):
        pl.semaphore_wait(barrier, near)
        tell_if(jnp.logical_and(above, jnp.logical_not(below)), rise, 1)
        tell_if(jnp.logical_and(below, jnp.logical_not(above)), fall, -1)

    def up1(p):
        lanes = pl.ds(p * CHUNK, CHUNK)
        return pltpu.make_async_remote_copy(
            src_ref=x_ref.at[pl.ds(rows - RATE, RATE), :, lanes],
            dst_ref=halo1.at[0, :, :, lanes],
            send_sem=h1_send.at[0, p],
            recv_sem=h1_recv.at[0, p],
            device_id={"space": sp + 1},
            device_id_type=MESH,
        )

    def down1(p):
        lanes = pl.ds(p * CHUNK, CHUNK)
        return pltpu.make_async_remote_copy(
            src_ref=x_ref.at[pl.ds(0, RATE), :, lanes],
            dst_ref=halo1.at[1, :, :, lanes],
            send_sem=h1_send.at[1, p],
            recv_sem=h1_recv.at[1, p],
            device_id={"space": sp - 1},
            device_id_type=MESH,
        )

    def up2(n):
        return pltpu.make_async_remote_copy(
            src_ref=edge2.at[0, n],
            dst_ref=halo2.at[0, n],
            send_sem=h2_send.at[0, n],
            recv_sem=h2_recv.at[0, n],
            device_id={"space": sp + 1},
            device_id_type=MESH,
        )

    def down2(n):
        return pltpu.make_async_remote_copy(
            src_ref=edge2.at[1, n],
            dst_ref=halo2.at[1, n],
            send_sem=h2_send.at[1, n],
            recv_sem=h2_recv.at[1, n],
            device_id={"space": sp - 1},
            device_id_type=MESH,
        )

    def send_rows(up, down, p):
        @pl.when(has_bot)
        def _():
            up(p).start()

        @pl.when(has_top)
        def _():
            down(p).start()

    def recv_rows(up, down, p):
        @pl.when(has_top)
        def _():
            up(p).wait_recv()

        @pl.when(has_bot)
        def _():
            down(p).wait_recv()

    def sent_rows(up, down, p):
        @pl.when(has_bot)
        def _():
            up(p).wait_send()

        @pl.when(has_top)
        def _():
            down(p).wait_send()

    for p in range(k_in):
        send_rows(up1, down1, p)

    for halo in (halo1, halo2):

        @pl.when(jnp.logical_not(has_top))
        def _():
            halo[0] = jnp.zeros(halo.shape[1:], BF16)

        @pl.when(jnp.logical_not(has_bot))
        def _():
            halo[1] = jnp.zeros(halo.shape[1:], BF16)

    def kind(i):
        if n_all > DIRECT:
            return "grid"
        if i in (at1, at2, at3, at3 + k_mid - 1):
            return "one"
        if at4 <= i < n_sum - ENDS or at2 + SLACK <= i < at3:
            return "grid"
        return "pair"

    def home(i):
        how = kind(i)
        if how == "one":
            return pb.at[i, self]
        return pa.at[i, pos_plane] if how == "grid" else pa.at[i, side]

    def hop(buf, i, slot, send, recv, device):
        return pltpu.make_async_remote_copy(
            src_ref=buf.at[i, slot],
            dst_ref=buf.at[i, slot],
            send_sem=send.at[i],
            recv_sem=recv.at[i],
            device_id=device,
            device_id_type=MESH,
        )

    def bulk(buf, i, count, send, recv, device):
        block = buf.at[i, pl.ds(0, count)]
        return pltpu.make_async_remote_copy(
            src_ref=block,
            dst_ref=block,
            send_sem=send.at[i],
            recv_sem=recv.at[i],
            device_id=device,
            device_id_type=MESH,
        )

    def near_all(i):
        if kind(i) == "grid":
            return bulk(pa, i, n_plane - 1, a_send, a_recv, plane(1))
        return bulk(pa, i, 1, a_send, a_recv, {"space": partner})

    def far_count(i):
        return {"one": n_all, "pair": n_far, "grid": n_z}[kind(i)]

    def far_all(i):
        device = {"one": other, "pair": far, "grid": line}[kind(i)](1)
        return bulk(pb, i, far_count(i) - 1, b_send, b_recv, device)

    def start(i):
        how = kind(i)
        if how == "one":
            each_other(lambda d: hop(pb, i, self, b_send, b_recv, other(d)).start())
        elif how == "grid":
            each(n_plane, lambda d: hop(pa, i, pos_plane, a_send, a_recv, plane(d)).start())
        else:
            hop(pa, i, side, a_send, a_recv, {"space": partner}).start()

    def relay(i):
        how = kind(i)
        if how == "one":
            return
        near_all(i).wait_recv()
        if how == "grid":
            s = pa[i, 0]
            for k in range(1, n_plane):
                s = s + pa[i, k]
            pb[i, pos_z] = s
            each(n_z, lambda d: hop(pb, i, pos_z, b_send, b_recv, line(d)).start())
        else:
            pb[i, mine] = pa[i, 0] + pa[i, 1]
            each(n_far, lambda d: hop(pb, i, mine, b_send, b_recv, far(d)).start())

    def finish(i):
        far_all(i).wait_recv()
        parts = [pb[i, k] for k in range(far_count(i))]
        while len(parts) > 1:
            parts = [a + b for a, b in zip(parts[0::2], parts[1::2])] + (
                parts[-1:] if len(parts) % 2 else []
            )
        s = parts[0] * (1.0 / total)
        mean = s[:PER]
        var = s[PER:] - mean * mean
        p = par[i]
        fac = p[:PER] * lax.rsqrt(var + EPS)
        coef[i, 0:PER] = fac
        coef[i, PER : 2 * PER] = p[PER:] - mean * fac

    def normal(v, i, q):
        return jnp.maximum(v * coef[i, pl.ds(q, 1), :] + coef[i, pl.ds(PER + q, 1), :], 0.0)

    def taps(d_ref, lanes):
        return [
            [d_ref[a, b : b + 1, lanes].astype(F32) for b in range(3)] for a in range(3)
        ]

    def conv_row(j, r, filt):
        y = None
        for a in range(3):
            for b in range(3):
                term = xp[j, r + RATE * a, pl.ds(PAD + RATE * (b - 1), cols), :] * filt[a][b]
                y = term if y is None else y + term
        return y

    def lanes_of(j):
        if isinstance(j, int):
            return slice(j * LANES, (j + 1) * LANES)
        return pl.ds(pl.multiple_of(j * LANES, LANES), LANES)

    def wide_of(n):
        if isinstance(n, int):
            return slice(n * CHUNK, (n + 1) * CHUNK)
        return pl.ds(pl.multiple_of(n * CHUNK, CHUNK), CHUNK)

    def fold(v):
        s = v[0:8]
        for k in range(1, v.shape[0] // 8):
            s = s + v[8 * k : 8 * k + 8]
        return s

    def conv_rows(j, row_list, d_ref, dst, s1, s2):
        lanes = lanes_of(j)
        filt = taps(d_ref, lanes)
        for r in row_list:
            y = conv_row(j, r, filt)
            dst[r * cols : (r + 1) * cols, lanes] = y
            s1 = s1 + fold(y)
            s2 = s2 + fold(y * y)
        return s1, s2

    def put_stats(i, q, s1, s2):
        to = home(i)
        to[pl.ds(q, 1), :] = jnp.sum(s1, axis=0, keepdims=True)
        to[pl.ds(PER + q, 1), :] = jnp.sum(s2, axis=0, keepdims=True)

    zero8 = jnp.zeros((8, LANES), F32)
    inner = list(range(RATE, rows - RATE))
    outer = list(range(RATE)) + list(range(rows - RATE, rows))

    def conv1_inner(j, carry):
        lanes = lanes_of(j)
        for r in range(rows):
            xp[j, r + RATE, PAD : PAD + cols, :] = x_ref[r, :, lanes].astype(F32)
        s1, s2 = conv_rows(j, inner, d1_ref, first, zero8, zero8)
        acc[0, j] = s1
        acc[1, j] = s2
        return carry

    for cp in load_small[:2]:
        cp.wait()
    for c in range(k_in):
        with scope("P03conv1inner"):
            load_inner(c).wait()
            lax.fori_loop(c * PER, (c + 1) * PER, conv1_inner, 0)
        with scope("P03meet"):
            meet(c)
    load_w1.start()
    load_w2.start()
    for cp in load_small[2:]:
        cp.wait()
    at = 0
    for g_ref, b_ref in ((g1_ref, b1_ref), (g2_ref, b2_ref), (g3_ref, b3_ref), (g4_ref, b4_ref)):
        for c in range(g_ref.shape[0] // CHUNK):
            for q in range(PER):
                lanes = slice(c * CHUNK + q * LANES, c * CHUNK + (q + 1) * LANES)
                par[at, q : q + 1, :] = g_ref[lanes].reshape(1, LANES)
                par[at, PER + q : PER + q + 1, :] = b_ref[lanes].reshape(1, LANES)
            at += 1

    def conv1_outer(i):
        def body(q, carry):
            j = i * PER + q
            lanes = lanes_of(j)
            for r in range(RATE):
                xp[j, r, PAD : PAD + cols, :] = halo1[0, r, :, lanes].astype(F32)
                xp[j, rows + RATE + r, PAD : PAD + cols, :] = halo1[1, r, :, lanes].astype(F32)
            s1, s2 = conv_rows(j, outer, d1_ref, first, acc[0, j], acc[1, j])
            put_stats(i, q, s1, s2)
            return carry

        return body

    for p in range(k_in):
        with scope("P04halo1wait"):
            recv_rows(up1, down1, p)
        with scope("P05conv1outer"):
            lax.fori_loop(0, PER, conv1_outer(p), 0)
            start(at1 + p)
        if p > 0:
            with scope("P06relay1"):
                relay(at1 + p - 1)
    with scope("P06relay1"):
        relay(at1 + k_in - 1)

    def norm_to(src, act, i, k):
        for b in range(pixels // step):
            span = slice(b * step, (b + 1) * step)
            for q in range(PER):
                lanes = lanes_of(k * PER + q)
                act[k, span, lanes_of(q)] = normal(src[span, lanes], i, q).astype(BF16)

    def tile(act, w_ref, dst, ks, n0, n1, fresh):
        wide = slice(n0 * CHUNK, n1 * CHUNK)
        y = None if fresh else dst[:, wide]
        for k in ks:
            z = jnp.dot(act[k], w_ref[wide_of(k), wide], preferred_element_type=F32)
            y = z if y is None else y + z
        dst[:, wide] = y
        return y

    def pairs(count):
        return [(n, min(n + WIDE, count)) for n in range(0, count, WIDE)]

    def tile_sums(i, s1, s2):
        for q in range(PER):
            part = slice(q * LANES, (q + 1) * LANES)
            put_stats(i, q, s1[:, part], s2[:, part])
        start(i)

    def groups(count, first_ones):
        at = 0
        for size in first_ones:
            if at + size < count:
                yield list(range(at, at + size))
                at += size
        yield list(range(at, count))

    for k in range(k_in):
        with scope("P07finish1"):
            finish(at1 + k)
        with scope("P08norm1"):
            norm_to(first, act1, at1 + k, k)
        if k == 0:
            load_w1.wait()
        with scope("P09mm1"):
            if k < k_in - 1:
                for n0, n1 in pairs(k_mid):
                    tile(act1, w1_ref, second, (k,), n0, n1, k == 0)
                continue
            for group in groups(k_mid, (1, 2)):
                sums = []
                for n in group:
                    y = tile(act1, w1_ref, second, (k,), n, n + 1, k == 0)
                    sums.append((at2 + n, fold(y), fold(y * y)))
                    edge2[0, n] = y[pixels - edge :].astype(BF16)
                    edge2[1, n] = y[:edge].astype(BF16)
                for s in sums:
                    tile_sums(*s)
    with scope("P10relay2"):
        for n in range(k_mid):
            relay(at2 + n)
            send_rows(up2, down2, n)

    def conv2(n):
        def body(q, carry):
            i = at2 + n
            j = n * PER + q
            lanes = lanes_of(j)
            part = lanes_of(q)
            for r in range(rows):
                v = normal(second[r * cols : (r + 1) * cols, lanes], i, q)
                xp[j, r + RATE, PAD : PAD + cols, :] = v
            top = normal(halo2[0, n, :, part].astype(F32), i, q)
            top = jnp.where(has_top, top, 0.0)
            bot = normal(halo2[1, n, :, part].astype(F32), i, q)
            bot = jnp.where(has_bot, bot, 0.0)
            for r in range(RATE):
                xp[j, r, PAD : PAD + cols, :] = top[r * cols : (r + 1) * cols]
                xp[j, rows + RATE + r, PAD : PAD + cols, :] = bot[r * cols : (r + 1) * cols]
            s1, s2 = conv_rows(j, list(range(rows)), d2_ref, second, zero8, zero8)
            put_stats(at3 + n, q, s1, s2)
            return carry

        return body

    for n in range(k_mid):
        with scope("P11finish2"):
            finish(at2 + n)
        with scope("P12edgewait"):
            recv_rows(up2, down2, n)
        with scope("P13conv2"):
            lax.fori_loop(0, PER, conv2(n), 0)
            start(at3 + n)
        with scope("P14relay3"):
            if n > 0:
                relay(at3 + n - 1)
    with scope("P14relay3"):
        relay(at3 + k_mid - 1)

    for k in range(k_mid):
        with scope("P15finish3"):
            finish(at3 + k)
        with scope("P16norm3"):
            norm_to(second, act3, at3 + k, k)
        if k == 0:
            load_w2.wait()
        with scope("P17mm2"):
            if k < k_mid - TAIL:
                for n0, n1 in pairs(k_out):
                    tile(act3, w2_ref, fourth, (k,), n0, n1, k == 0)
            if k == k_mid - 1:
                last_ks = tuple(range(max(k_mid - TAIL, 0), k_mid))
                for group in groups(k_out, (4,)):
                    sums = []
                    for n in group:
                        y = tile(act3, w2_ref, fourth, last_ks, n, n + 1, last_ks[0] == 0)
                        sums.append((at4 + n, fold(y), fold(y * y)))
                    for s in sums:
                        tile_sums(*s)
    with scope("P18relay4"):
        for n in list(range(k_out - ENDS, k_out)) + list(range(k_out - ENDS)):
            relay(at4 + n)

    def last(n, carry):
        i = at4 + n
        finish(i)
        for q in range(PER):
            lanes = lanes_of(n * PER + q)
            for b in range(pixels // step):
                span = slice(b * step, (b + 1) * step)
                out[span, lanes] = normal(fourth[span, lanes], i, q).astype(BF16)
        return carry

    with scope("P19last"):
        for n in list(range(3)) + list(range(k_out - ENDS, k_out)) + list(range(3, k_out - ENDS)):
            last(n, 0)

    with scope("P20drain"):
        for p in range(k_in):
            sent_rows(up1, down1, p)
        for n in range(k_mid):
            sent_rows(up2, down2, n)
        for i in range(n_sum):
            if kind(i) != "one":
                near_all(i).wait_send()
            far_all(i).wait_send()


def per_device(
    features,
    depth_one,
    gain_one,
    shift_one,
    point_one,
    gain_two,
    shift_two,
    depth_two,
    gain_three,
    shift_three,
    point_two,
    gain_four,
    shift_four,
):
    samples, span_rows, cols, c_in = features.shape
    rows = samples * span_rows
    assert samples == 1
    c_mid = point_one.shape[1]
    c_out = point_two.shape[1]
    pixels = rows * cols
    n_space = lax.axis_size("space")
    n_batch = lax.axis_size("batch")
    k_in, k_mid, k_out = c_in // CHUNK, c_mid // CHUNK, c_out // CHUNK
    n_sum = k_in + 2 * k_mid + k_out
    n_all = n_batch * n_space
    slots = n_all if n_all <= DIRECT else n_batch // lines_of(n_batch)
    any_spec = pl.BlockSpec(memory_space=pl.ANY)
    vmem = pl.BlockSpec(memory_space=pltpu.VMEM)
    edge = RATE * cols
    DMA = pltpu.SemaphoreType.DMA
    out = pl.pallas_call(
        functools.partial(kernel, n_space, n_batch),
        out_shape=pltpu.VMEM((pixels, c_out), BF16),
        in_specs=[any_spec] * 13,
        out_specs=vmem,
        scratch_shapes=[
            pltpu.VMEM(depth_one.shape, BF16),
            pltpu.VMEM(depth_two.shape, BF16),
        ]
        + [pltpu.VMEM((c,), F32) for c in (c_in, c_in, c_mid, c_mid, c_mid, c_mid, c_out, c_out)]
        + [
            pltpu.VMEM((rows, cols, c_in), BF16),
            pltpu.VMEM((c_in, c_mid), BF16),
            pltpu.VMEM((c_mid, c_out), BF16),
            pltpu.VMEM((2, RATE, cols, c_in), BF16),
            pltpu.VMEM((2, k_mid, edge, CHUNK), BF16),
            pltpu.VMEM((2, k_mid, edge, CHUNK), BF16),
            pltpu.VMEM((c_mid // LANES, rows + 2 * RATE, cols + 2 * PAD, LANES), F32),
            pltpu.VMEM((pixels, c_in), F32),
            pltpu.VMEM((k_in, pixels, CHUNK), BF16),
            pltpu.VMEM((pixels, c_mid), F32),
            pltpu.VMEM((k_mid, pixels, CHUNK), BF16),
            pltpu.VMEM((pixels, c_out), F32),
            pltpu.VMEM((n_sum, 2 * PER, LANES), F32),
            pltpu.VMEM((n_sum, 2 * PER, LANES), F32),
            pltpu.VMEM((2, c_in // LANES, 8, LANES), F32),
            pltpu.VMEM((n_sum, lines_of(n_batch) * n_space, 2 * PER, LANES), F32),
            pltpu.VMEM((n_sum, slots, 2 * PER, LANES), F32),
            DMA((2 + k_in,)),
            DMA((2,)),
            DMA((10,)),
            DMA((2, k_in)),
            DMA((2, k_in)),
            DMA((2, k_mid)),
            DMA((2, k_mid)),
            DMA((n_sum,)),
            DMA((n_sum,)),
            DMA((n_sum,)),
            DMA((n_sum,)),
            pltpu.SemaphoreType.REGULAR,
            pltpu.SemaphoreType.REGULAR,
        ],
        compiler_params=pltpu.CompilerParams(
            collective_id=0, has_side_effects=True, vmem_limit_bytes=56 * 1024 * 1024
        ),
        name="exit_block",
    )(
        features.reshape(rows, cols, c_in),
        point_one,
        point_two,
        depth_one,
        depth_two,
        gain_one,
        shift_one,
        gain_two,
        shift_two,
        gain_three,
        shift_three,
        gain_four,
        shift_four,
    )
    return out.reshape(samples, span_rows, cols, c_out)


def solution(mesh):
    return jax.shard_map(
        per_device,
        mesh=mesh,
        in_specs=(P("batch", "space", None, None),) + (P(),) * 12,
        out_specs=P("batch", "space", None, None),
        check_vma=False,
    )
```
